32 devices in a mesh: lat: 4 (over y, core), lon: 4 (over z), lev: 2 (over x).
Axes of the slice: x: 2, y: 2, z: 4, core: 2. Of those that a mesh axis runs over, the one named last changes fastest.
Arguments:
- density: float32 [128, 16, 256, 128], P('lat', 'lon', 'lev'), may hold values from 0.2 to 1.8
- crowding: float32 [128, 16, 256, 128], P('lat', 'lon', 'lev'), may hold values from 0.5 to 2
Outputs:
- running_total: float32 [128, 16, 256, 128], P('lat', 'lon', 'lev')
- density_end: float32 [128, 16, 256, 128], P('lat', 'lon', 'lev')
The draws below stay inside these ranges and needn't reach their ends.
All inputs are finite; a program needn't handle non-finite values.
Results may differ from the reference program's by a relative error of at most 0.00002.
Values sent between devices are 32-bit elements; how exact they have to be, the bound alone decides.
No kernel may reach another device: no remote copies, remote signals or barrier semaphores. Data moves between devices by JAX's collectives and lax.ppermute only.
A program may use at most 320 MiB of HBM per device.

```python
import jax
import jax.numpy as jnp
from jax import lax

GRID_J = 128
GRID_I = 16
GRID_K = 256
LEVELS = 128
STEPS = 4


def level_of(stream_key, shape, split, smallest, largest):
    level, own = 1.0, jax.random.fold_in(stream_key, 6)
    for dim, shards_of in split:
        heights = jnp.exp(jax.random.uniform(jax.random.fold_in(own, dim), (shards_of,), jnp.float32, smallest / len(split), largest / len(split)))
        level = level * jnp.repeat(heights, shape[dim] // shards_of).reshape([-1 if axis == dim else 1 for axis in range(len(shape))])
    return level


def setup_inputs(seed: int = 0) -> dict:
    key_list = jax.random.split(jax.random.key(seed), 3)
    density = jnp.clip(0.2 + 1.5999999 * jax.random.uniform(key_list[0], (GRID_J, GRID_I, GRID_K, LEVELS), jnp.float32) ** level_of(key_list[0], (GRID_J, GRID_I, GRID_K, LEVELS), ((0, 4), (1, 4), (2, 2)), -0.2, 0.2), 0.2, 1.8)
    crowding = jnp.clip(0.5 + 1.5 * jax.random.uniform(key_list[1], (GRID_J, GRID_I, GRID_K, LEVELS), jnp.float32) ** level_of(key_list[1], (GRID_J, GRID_I, GRID_K, LEVELS), ((0, 4), (1, 4), (2, 2)), -0.2, 0.2), 0.5, 2.0)
    return dict(density=density, crowding=crowding)


def without_rim(values, dims):
    for dim in dims:
        values = lax.slice_in_dim(values, 1, values.shape[dim] - 1, axis=dim)
    return values


def shifted_cells(values, dim, start, dims):
    others = [other for other in dims if other != dim]
    values = without_rim(values, others)
    return lax.slice_in_dim(values, start, start + values.shape[dim] - 2, axis=dim)


def march_step(padded, crowding):
    middle = without_rim(padded, (0, 1, 2))
    lower = [shifted_cells(padded, dim, 0, (0, 1, 2)) for dim in (0, 1, 2)]
    upper = [shifted_cells(padded, dim, 2, (0, 1, 2)) for dim in (0, 1, 2)]
    spread = lower[0] + upper[0] + lower[1] + upper[1] + lower[2] + upper[2] - 6.0 * middle
    return middle + 0.1 * spread + 0.2 * middle * (1.0 - middle * crowding)


def reference(density, crowding):
    for step in range(STEPS):
        density = march_step(jnp.pad(density, ((1, 1), (1, 1), (1, 1), (0, 0)), mode="wrap"), crowding)
    running_total = jnp.cumsum(density, axis=1) / GRID_I
    return running_total, density
```

```python
import functools

import jax
import jax.numpy as jnp
from jax import lax
from jax.experimental import pallas as pl
from jax.experimental.pallas import tpu as pltpu
from jax.sharding import PartitionSpec as P

STEPS = 4
CHUNKS = 4


def rows_per_block(rows, row_bytes):
    block = 1
    while rows % (2 * block) == 0 and 2 * block * row_bytes <= 2**20:
        block *= 2
    return block


def step_kernel(*refs, block, cells, last, top, bottom, ordered):
    mid, prev, nxt, up, down, lon_lo, lon_hi, lev_lo, lev_hi, crowd = refs[:10]
    outs = list(refs[10 + ordered :])
    new = outs.pop(0)
    if last:
        total = outs.pop(0)
    else:
        first_face, last_face, lev_first, lev_last = outs[:4]
        outs = outs[4:]
        top_row = outs.pop(0) if top else None
        bottom_row = outs.pop(0) if bottom else None
    g = pl.program_id(0)
    at_start = g == 0
    at_end = g == pl.num_programs(0) - 1
    depth = mid.shape[2]
    k = lax.broadcasted_iota(jnp.int32, mid.shape[2:], 0)
    for r in range(block):
        acc = None
        for i in range(cells):
            x = mid[r, i]
            above = mid[r - 1, i] if r > 0 else jnp.where(at_start, up[0, i], prev[0, i])
            below = mid[r + 1, i] if r + 1 < block else jnp.where(at_end, down[0, i], nxt[0, i])
            left = mid[r, i - 1] if i > 0 else lon_lo[r]
            right = mid[r, i + 1] if i + 1 < cells else lon_hi[r]
            lo = jnp.where(k == 0, lev_lo[r, i : i + 1], pltpu.roll(x, 1, 0))
            hi = jnp.where(k == depth - 1, lev_hi[r, i : i + 1], pltpu.roll(x, depth - 1, 0))
            spread = above + below + left + right + lo + hi - 6.0 * x
            y = x + 0.1 * spread + 0.2 * x * (1.0 - x * crowd[r, i])
            new[r, i] = y
            if last:
                acc = y if acc is None else acc + y
            else:
                if i == 0:
                    first_face[r] = y
                if i == cells - 1:
                    last_face[r] = y
                lev_first[r, i : i + 1] = y[0:1]
                lev_last[r, i : i + 1] = y[depth - 1 : depth]
        if last:
            total[r] = acc
    if not last:
        if top:

            @pl.when(at_start)
            def _():
                top_row[0] = new[0]

        if bottom:

            @pl.when(at_end)
            def _():
                bottom_row[0] = new[block - 1]


def step_chunk(source, base, up, down, lon, lev, crowding, crowd_base, rows, last, top, bottom, order):
    cells, depth, levels = source.shape[1:]
    block = rows_per_block(rows, cells * depth * levels * 4)
    grid = rows // block
    final = source.shape[0] - 1
    row = (1, cells, depth, levels)

    def at_row(index):
        return pl.BlockSpec(row, lambda g: (index(g), 0, 0, 0))

    whole = pl.BlockSpec((block, cells, depth, levels), lambda g: (g, 0, 0, 0))
    face = pl.BlockSpec((block, depth, levels), lambda g: (g, 0, 0))
    edge = pl.BlockSpec((block, cells, levels), lambda g: (g, 0, 0))
    fixed = pl.BlockSpec(row, lambda g: (0, 0, 0, 0))
    in_specs = [
        pl.BlockSpec((block, cells, depth, levels), lambda g: (base // block + g, 0, 0, 0)),
        at_row(lambda g: jnp.maximum(base + g * block - 1, 0)),
        at_row(lambda g: jnp.minimum(base + g * block + block, final)),
        at_row(lambda g: up[1]),
        at_row(lambda g: down[1]),
        face,
        face,
        edge,
        edge,
        pl.BlockSpec((block, cells, depth, levels), lambda g: (crowd_base // block + g, 0, 0, 0)),
    ]
    operands = [source, source, source, up[0], down[0], lon[0], lon[1], lev[0], lev[1], crowding]
    if order is not None:
        in_specs.append(pl.BlockSpec(memory_space=pl.ANY))
        operands.append(order)
    f32 = jnp.float32
    out_specs = [whole]
    out_shape = [jax.ShapeDtypeStruct((rows, cells, depth, levels), f32)]
    if last:
        out_specs.append(face)
        out_shape.append(jax.ShapeDtypeStruct((rows, depth, levels), f32))
    else:
        out_specs += [face, face, edge, edge]
        out_shape += [jax.ShapeDtypeStruct((rows, depth, levels), f32)] * 2
        out_shape += [jax.ShapeDtypeStruct((rows, cells, levels), f32)] * 2
        for wanted in (top, bottom):
            if wanted:
                out_specs.append(fixed)
                out_shape.append(jax.ShapeDtypeStruct(row, f32))
    return pl.pallas_call(
        functools.partial(
            step_kernel, block=block, cells=cells, last=last, top=top, bottom=bottom, ordered=int(order is not None)
        ),
        grid=(grid,),
        in_specs=in_specs,
        out_specs=out_specs,
        out_shape=out_shape,
        compiler_params=pltpu.CompilerParams(dimension_semantics=("arbitrary",)),
    )(*operands)


def finish_kernel(*refs, block, cells, scale):
    values, below = refs[:2]
    running, end = refs[-2:]
    for r in range(block):
        total = below[r]
        for i in range(cells):
            y = values[r, i]
            total = total + y
            running[r, i] = total * scale
            end[r, i] = y


def finish_chunk(values, below, into, base, full, scale):
    rows, cells, depth, levels = values.shape
    block = rows_per_block(rows, cells * depth * levels * 4)
    whole = (block, cells, depth, levels)
    placed = pl.BlockSpec(whole, lambda g: (base // block + g, 0, 0, 0))
    in_specs = [
        pl.BlockSpec(whole, lambda g: (g, 0, 0, 0)),
        pl.BlockSpec((block, depth, levels), lambda g: (g, 0, 0)),
    ]
    operands = [values, below]
    aliases = {}
    if into is not None:
        in_specs += [pl.BlockSpec(memory_space=pl.ANY)] * 2
        operands += list(into)
        aliases = {2: 0, 3: 1}
    return pl.pallas_call(
        functools.partial(finish_kernel, block=block, cells=cells, scale=scale),
        grid=(rows // block,),
        in_specs=in_specs,
        out_specs=[placed, placed],
        out_shape=[jax.ShapeDtypeStruct(full, jnp.float32)] * 2,
        input_output_aliases=aliases,
        compiler_params=pltpu.CompilerParams(dimension_semantics=("arbitrary",)),
    )(*operands)


def from_below(value, axis):
    count = lax.axis_size(axis)
    return lax.ppermute(value, axis, [(i, (i + 1) % count) for i in range(count)])


def from_above(value, axis):
    count = lax.axis_size(axis)
    return lax.ppermute(value, axis, [((i + 1) % count, i) for i in range(count)])


def body(density, crowding):
    full = density.shape
    rows_all, cells = full[:2]
    chunks = CHUNKS if rows_all % CHUNKS == 0 else 1
    rows = rows_all // chunks
    count = lax.axis_size("lon")

    def part(values, c):
        return lax.slice_in_dim(values, c * rows, (c + 1) * rows, axis=0)

    first, final = density[:, 0], density[:, cells - 1]
    lev_first, lev_last = density[:, :, 0], density[:, :, full[2] - 1]
    faces = [(part(first, c), part(final, c), part(lev_first, c), part(lev_last, c)) for c in range(chunks)]
    top, bottom = density[:1], density[rows_all - 1 :]
    fields = [(density, c * rows) for c in range(chunks)]
    order = None
    totals = []
    for step in range(STEPS):
        last = step == STEPS - 1
        lat = (from_below(bottom, "lat"), from_above(top, "lat"))
        halos = []
        for head, tail, lev_head, lev_tail in faces:
            lon = (from_below(tail, "lon"), from_above(head, "lon"))
            lev = (from_below(lev_tail, "lev"), from_above(lev_head, "lev"))
            halos.append((lon, lev))
        made = []
        for c in range(chunks):
            source, base = fields[c]
            up = (fields[c - 1][0], fields[c - 1][1] + rows - 1) if c > 0 else (lat[0], 0)
            down = fields[c + 1] if c + 1 < chunks else (lat[1], 0)
            lon, lev = halos[c]
            outs = step_chunk(
                source, base, up, down, lon, lev, crowding, c * rows, rows, last, c == 0, c == chunks - 1, order
            )
            order = outs[0]
            made.append(outs)
        fields = [(outs[0], 0) for outs in made]
        if last:
            totals = [outs[1] for outs in made]
        else:
            faces = [tuple(outs[1:5]) for outs in made]
            top, bottom = made[0][5], made[-1][-1]
    into = None
    for c in range(chunks):
        below = jnp.zeros_like(totals[c])
        for hop in range(count - 1):
            arrived = lax.ppermute(below + totals[c], "lon", [(hop, hop + 1)])
            below = below + arrived
        into = finish_chunk(fields[c][0], below, into, c * rows, full, 1.0 / (cells * count))
    return tuple(into)


def solution(mesh):
    spec = P("lat", "lon", "lev", None)
    return jax.shard_map(body, mesh=mesh, in_specs=(spec, spec), out_specs=(spec, spec), check_vma=False)
```
